128 devices in a mesh: var: 32 (over y, z, core), samp: 4 (over x).
Axes of the slice: x: 4, y: 4, z: 4, core: 2. Of those that a mesh axis runs over, the one named last changes fastest.
Arguments:
- genotypes: bfloat16 [49152, 16384], P('samp', 'var'), may hold values from -4 to 4
- labels: int32 [49152, 256], P(('samp', 'var')), may hold values 0 or 1
- act_coef: bfloat16 [16, 8192], P(None, 'var'), may hold values from -0.125 to 0.125
- act_index: int32 [8192], P('var'), may hold values from 0 to 511, as said below
- act_count: int32 [32], P('var'), may hold values from 1 to 256, as said below
- loadings: float32 [16, 256], replicated, may hold values from -1.5 to 1.5
- intercept: float32 [256], replicated, may hold values from -2.5 to 0.5
Outputs:
- grad_var: float32 [16, 16384], P(None, 'var')
- grad_trait: float32 [16, 256], replicated
- inactive_score: float32 [16384], P('var')
- top_score: float32 [1], replicated
The draws below stay inside these ranges and needn't reach their ends.
Inputs may be any that keep to these rules, and one draw needn't show every extreme that they name: `act_index`: within each aligned block of 256 slots (one index of var) the numbers are distinct; slots past that block's count are padding and carry no variant. `act_count`: some index of var has all 256 slots live.
All inputs are finite; a program needn't handle non-finite values. No bound on the sum of `labels` on one device may be relied on, other than what follows from the above.
Results may differ from the reference program's by a relative error of at most 0.0033.
Values may be sent and summed in bfloat16 or wider, within the bound.
A program may use at most 64 MiB of HBM per device.

```python
import math
import jax
import jax.numpy as jnp
from jax import lax

TRAITS = 256
RANK = 16
VAR_DEV = 512
ACT_MAX = 256
SAMPLES = 49152
VARIANTS = 16384
ACT_ROWS = 8192
N_VAR = 32


def draw_act_index(key, part):
    shards = ACT_ROWS // ACT_MAX
    keys = jax.random.split(jax.random.fold_in(key, 11), shards)

    def one_shard(sub):
        return jax.random.permutation(sub, VAR_DEV)[:ACT_MAX].astype(jnp.int32)
    return jax.vmap(one_shard)(keys).reshape(-1).astype(jnp.int32)


def draw_act_count(key, part):
    shards = ACT_ROWS // ACT_MAX
    first = jax.random.randint(jax.random.fold_in(key, 21), (shards,), 0, ACT_MAX)
    second = jax.random.randint(jax.random.fold_in(key, 22), (shards,), 0, ACT_MAX)
    counts = 1 + first * second // ACT_MAX
    busiest = jax.random.randint(jax.random.fold_in(key, 23), (), 0, shards)
    return jnp.where(jnp.arange(shards) == busiest, ACT_MAX, counts).astype(jnp.int32)


def with_ends(entries, rng, low, high):
    dims = entries.shape
    place = [jax.random.randint(jax.random.fold_in(rng, axis), (), 0, dims[axis]) for axis in range(len(dims))]
    entries = entries.at[tuple(place)].set(low)
    longest = dims.index(max(dims))
    place[longest] = (place[longest] + 1) % dims[longest]
    return entries.at[tuple(place)].set(high)


def block_levels(key, dims, cuts, smallest, top_value):
    level = 1.0
    for axis_at, shards_of in cuts:
        heights = jax.random.uniform(jax.random.fold_in(jax.random.fold_in(key, 6), axis_at), (shards_of,), jnp.float32, smallest / len(cuts), top_value / len(cuts))
        level = level * jnp.repeat(jnp.exp(heights), dims[axis_at] // shards_of).reshape((-1,) + (1,) * (len(dims) - 1 - axis_at))
    return level


def gaussian(stream_key, extent, spread, bound, pieces=(), kind=jnp.bfloat16):
    array = jax.random.normal(stream_key, extent, jnp.float32) * spread
    if len(pieces) > 0:
        array = block_levels(stream_key, extent, pieces, -0.22, 0.18) * array
    return jnp.clip(array, min=-bound, max=bound).astype(kind)


def setup_inputs(seed: int = 0) -> dict:
    splits = jax.random.split(jax.random.key(seed), 8)
    return {
        "genotypes": gaussian(splits[0], (SAMPLES, VARIANTS), 1.0, 4.0, ((0, 4), (1, 32))),
        "labels": with_ends((jax.random.randint(splits[1], (SAMPLES, TRAITS), 0, 4) < 1).astype(jnp.int32), jax.random.fold_in(splits[1], 1), 0, 1),
        "act_coef": gaussian(splits[2], (RANK, ACT_ROWS), (ACT_MAX * N_VAR // 4) ** -0.5, 0.125, ((1, 32),)),
        "act_index": draw_act_index(jax.random.fold_in(splits[7], 71), 0),
        "act_count": draw_act_count(jax.random.fold_in(splits[7], 71), 0),
        "loadings": gaussian(splits[5], (RANK, TRAITS), RANK ** -0.5, 1.5, (), jnp.float32),
        "intercept": jnp.clip(jax.random.uniform(splits[6], (TRAITS,), jnp.float32, -2.5, 0.5), -2.5, 0.5),
    }


def reference(genotypes, labels, act_coef, act_index, act_count, loadings, intercept):
    slots = jnp.arange(ACT_ROWS, dtype=jnp.int32)
    owner = (slots // ACT_MAX).astype(jnp.int32)
    live = slots % ACT_MAX < act_count[owner]
    column = (act_index + owner * VAR_DEV).astype(jnp.int32)
    picked = jnp.where(live[None, :], act_coef.astype(jnp.float32), jnp.float32(0.0))
    coef = jnp.zeros((RANK, VARIANTS), jnp.float32).at[:, column].add(picked).astype(jnp.bfloat16)
    active = jnp.zeros((VARIANTS,), jnp.float32).at[column].add(live.astype(jnp.float32))
    predictor = lax.dot_general(coef, genotypes, (((1,), (1,)), ((), ())), preferred_element_type=jnp.float32)
    eta = jnp.einsum('rs,rt->st', predictor, loadings, precision=lax.Precision.HIGHEST) + intercept[None, :]
    resid = jax.nn.sigmoid(eta) - labels.astype(jnp.float32)
    weights = jnp.einsum('rt,st->rs', loadings, resid, precision=lax.Precision.HIGHEST).astype(jnp.bfloat16)
    norm = 1.0 / math.sqrt(SAMPLES)
    grad_var = jnp.dot(weights, genotypes, preferred_element_type=jnp.float32) * norm
    grad_trait = jnp.einsum('rs,st->rt', predictor, resid, precision=lax.Precision.HIGHEST) * norm
    score = jnp.sqrt(lax.optimization_barrier(jnp.sum(grad_var * grad_var, axis=0)))
    inactive_score = jnp.where(active > 0, jnp.float32(0.0), score)
    top_score = jnp.max(inactive_score)[None]
    return (grad_var, grad_trait, inactive_score, top_score)
```

```python
import functools
import math

import jax
import jax.numpy as jnp
from jax import lax
from jax.experimental import pallas as pl
from jax.experimental.pallas import tpu as pltpu
from jax.sharding import PartitionSpec as P

MESH = pl.DeviceIdType.MESH
F32 = jnp.float32
BF16 = jnp.bfloat16
SIDE = 4
CHIPS = SIDE * SIDE
XS = 4
NT = (((1,), (1,)), ((), ()))
TN = (((0,), (0,)), ((), ()))
NN = (((1,), (0,)), ((), ()))


def div(a, b):
    return lax.div(a, jnp.int32(b))


def rem(a, b):
    return lax.rem(a, jnp.int32(b))


def stride(i):
    return rem(10 - div(i * (i + 1), 2), SIDE)


def dot(a, b, dims):
    return lax.dot_general(a, b, dims, preferred_element_type=F32)


def halves(x):
    high = x.astype(BF16)
    return high, (x - high.astype(F32)).astype(BF16)


def kernel(
    norm, geno_hbm, labels_hbm, coef_hbm, index_hbm, count_hbm, load_hbm, icpt_hbm,
    gv_ref, gt_ref, score_ref, top_ref,
    geno, labels, coef, index, count, load, icpt,
    pair_out, pair_in, pred_out, pred_in, w_same, w_pair, vp, tops,
    tr_own, tr_core, tr_x, tr_y, tr_z,
    geno_sem, small_sem, pair_send, pair_recv, pred_send, pred_recv,
    w_send, w_recv, relay_send, relay_recv, vp_send, vp_recv, top_send, top_recv,
    tr_send, tr_core_recv, tr_x_recv, tr_y_recv, tr_z_recv,
):
    me = lax.axis_index("var")
    samp = lax.axis_index("samp")
    core = rem(me, 2)
    chip = div(me, 2)
    y, z = div(chip, SIDE), rem(chip, SIDE)
    other = 1 - core
    partner = chip * 2 + other

    def to_chip(i):
        return rem(y + stride(div(i, SIDE)), SIDE) * SIDE + rem(z + stride(rem(i, SIDE)), SIDE)

    def from_chip(i):
        return rem(y + SIDE - stride(div(i, SIDE)), SIDE) * SIDE + rem(
            z + SIDE - stride(rem(i, SIDE)), SIDE
        )

    def send(src, dst, send_sem, recv_sem, var, samp_at):
        return pltpu.make_async_remote_copy(
            src_ref=src,
            dst_ref=dst,
            send_sem=send_sem,
            recv_sem=recv_sem,
            device_id=(var, samp_at),
            device_id_type=MESH,
        )

    small = [
        pltpu.make_async_copy(src, dst, small_sem.at[k])
        for k, (src, dst) in enumerate(
            (
                (index_hbm, index),
                (count_hbm, count),
                (coef_hbm, coef),
                (load_hbm, load),
                (icpt_hbm, icpt),
                (labels_hbm, labels),
            )
        )
    ]
    for copy in small[:5]:
        copy.start()
    rows = labels.shape[0]

    def geno_copy(i, which):
        at = to_chip(i) * 2 + which
        return pltpu.make_async_copy(
            geno_hbm.at[pl.ds(pl.multiple_of(at * rows, rows), rows)], geno.at[at], geno_sem.at[at]
        )

    def start_geno(i, carry, which):
        geno_copy(i, which).start()
        return carry

    lax.fori_loop(0, CHIPS, functools.partial(start_geno, which=other), 0)
    lax.fori_loop(0, CHIPS, functools.partial(start_geno, which=core), 0)
    small[5].start()

    barrier = pltpu.get_barrier_semaphore()

    def greet(i, carry):
        for which in range(2):
            pl.semaphore_signal(
                barrier, inc=1, device_id=(to_chip(i) * 2 + which, samp), device_id_type=MESH
            )
        return carry

    lax.fori_loop(0, CHIPS - 1, greet, 0)
    pl.semaphore_signal(barrier, inc=1, device_id=(partner, samp), device_id_type=MESH)
    for step in range(1, XS):
        pl.semaphore_signal(
            barrier, inc=1, device_id=(me, rem(samp + step, XS)), device_id_type=MESH
        )

    for copy in small[:5]:
        copy.wait()
    slots = index.shape[1]
    width = geno.shape[2]
    lane = lax.broadcasted_iota(jnp.int32, (1, slots), 1)
    live = lane < count[...]
    variant = lax.broadcasted_iota(jnp.int32, (width, slots), 0)
    chosen = jnp.where((variant == index[...]) & live, F32(1.0), F32(0.0)).astype(BF16)
    dense = dot(coef[...], chosen, NT).astype(BF16)
    active = dot(jnp.where(live, F32(1.0), F32(0.0)).astype(BF16), chosen, NT)

    def for_partner(k, carry):
        for u in range(2):
            i = k * 2 + u
            geno_copy(i, other).wait()
        for u in range(2):
            i = k * 2 + u
            part = dot(dense, geno[to_chip(i) * 2 + other], NT)
            pair_out[i] = part.astype(BF16)
        return carry

    lax.fori_loop(0, CHIPS // 2, for_partner, 0)

    pl.semaphore_wait(barrier, 2 * CHIPS - 1 + XS - 1)
    to_pair = send(pair_out, pair_in, pair_send, pair_recv, partner, samp)
    to_pair.start()

    def pred_copy(i):
        return send(
            pred_out.at[i],
            pred_in.at[i],
            pred_send.at[i],
            pred_recv.at[i],
            to_chip(i) * 2 + core,
            samp,
        )

    to_pair.wait_recv()

    def for_same(k, carry):
        for u in range(2):
            i = k * 2 + u
            geno_copy(i, core).wait()
        for u in range(2):
            i = k * 2 + u
            part = dot(dense, geno[to_chip(i) * 2 + core], NT)
            pred_out[i] = (part + pair_in[i].astype(F32)).astype(BF16)
            pred_copy(i).start()
        return carry

    lax.fori_loop(0, CHIPS // 2 - 1, for_same, 0)
    last = CHIPS - 2
    geno_copy(last, core).wait()
    part = dot(dense, geno[to_chip(last) * 2 + core], NT)
    pred_out[last] = (part + pair_in[last].astype(F32)).astype(BF16)
    pred_copy(last).start()
    geno_copy(CHIPS - 1, core).wait()
    mine = dot(dense, geno[me], NT) + pair_in[CHIPS - 1].astype(F32)

    small[5].wait()
    load_h, load_m = halves(load[...])
    load_both = jnp.concatenate([load_h, load_m], axis=0)

    def add_pred(k, total):
        i = CHIPS - 2 - k
        pred_copy(i).wait_recv()
        return total + pred_in[i].astype(F32)

    mine = lax.fori_loop(0, CHIPS - 1, add_pred, mine)
    mine_h, mine_m = halves(mine)
    eta = (
        dot(
            jnp.concatenate([mine_h, mine_h, mine_m], axis=0),
            jnp.concatenate([load_h, load_m, load_h], axis=0),
            TN,
        )
        + icpt[...]
    )
    resid = 1.0 / (1.0 + jnp.exp(-eta)) - labels[...].astype(F32)
    resid_h, resid_m = halves(resid)
    first = dot(load_both, resid_h, NT)
    rank = load.shape[0]
    weights = first[:rank] + first[rank:] + dot(load_h, resid_m, NT)
    w_same[CHIPS - 1] = weights.astype(BF16)

    def w_copy(i):
        return send(
            w_same.at[CHIPS - 1],
            w_same.at[i],
            w_send.at[i],
            w_recv.at[i],
            to_chip(i) * 2 + core,
            samp,
        )

    def relay_copy(i):
        return send(
            w_same.at[i], w_pair.at[i], relay_send.at[i], relay_recv.at[i], partner, samp
        )

    def start_w(i, carry):
        w_copy(i).start()
        return carry

    lax.fori_loop(0, CHIPS - 1, start_w, 0)
    relay_copy(CHIPS - 1).start()

    both = dot(jnp.concatenate([mine_h, mine_m], axis=0), resid_h, NN)
    tr_own[...] = (both[:rank] + both[rank:] + dot(mine_h, resid_m, NN)) * norm
    tr_core_copy = send(tr_own, tr_core, tr_send.at[0], tr_core_recv, partner, samp)
    tr_core_copy.start()

    def same_block(i, total):
        w_copy(i).wait_recv()
        relay_copy(i).start()
        return total + dot(w_same[i], geno[from_chip(i) * 2 + core], NN)

    def pair_block(i, total):
        relay_copy(i).wait_recv()
        return total + dot(w_pair[i], geno[from_chip(i) * 2 + other], NN)

    def ring_copies(slots, at, send_base, recv_sems, where):
        return [
            send(
                slots.at[at],
                slots.at[at],
                tr_send.at[send_base + step - 1],
                recv_sems.at[at],
                *where(step),
            )
            for step in range(1, SIDE)
        ]

    def ring_start(value, slots, at, send_base, recv_sems, where):
        slots[at] = value
        copies = ring_copies(slots, at, send_base, recv_sems, where)
        for copy in copies:
            copy.start()
        return copies

    def ring_sum(slots, at, recv_sems, where):
        for step in range(1, SIDE):
            source = rem(at + step, SIDE)
            send(
                slots.at[source], slots.at[source], tr_send.at[0], recv_sems.at[source], *where(1)
            ).wait_recv()
        return (slots[0] + slots[1]) + (slots[2] + slots[3])

    def along_x(step):
        return me, rem(samp + step, XS)

    def along_y(step):
        return (rem(y + step, SIDE) * SIDE + z) * 2 + core, samp

    def along_z(step):
        return (y * SIDE + rem(z + step, SIDE)) * 2 + core, samp

    def blocks(low, high, total):
        def block(k, total):
            i = high - 1 - k
            total = same_block(i, total)
            return pair_block(i + 1, total)

        return lax.fori_loop(0, high - low, block, total)

    total = dot(w_same[CHIPS - 1], geno[me], NN)
    total = blocks(11, 15, total)
    tr_core_copy.wait_recv()
    x_copies = ring_start(tr_own[...] + tr_core[...], tr_x, samp, 1, tr_x_recv, along_x)
    total = blocks(5, 11, total)
    x_total = ring_sum(tr_x, samp, tr_x_recv, along_x)
    y_copies = ring_start(x_total, tr_y, y, 4, tr_y_recv, along_y)
    total = blocks(0, 5, total)
    total = pair_block(0, total)

    vp[samp] = total.astype(BF16)

    def vp_copy(step):
        return send(
            vp.at[samp],
            vp.at[samp],
            vp_send.at[step - 1],
            vp_recv.at[samp],
            me,
            rem(samp + step, XS),
        )

    for step in range(1, XS):
        vp_copy(step).start()
    y_total = ring_sum(tr_y, y, tr_y_recv, along_y)
    z_copies = ring_start(y_total, tr_z, z, 7, tr_z_recv, along_z)
    for step in range(1, XS):
        source = rem(samp + step, XS)
        send(
            vp.at[source], vp.at[source], vp_send.at[0], vp_recv.at[source], me, rem(samp + 1, XS)
        ).wait_recv()
    grad = vp[0].astype(F32)
    for source in range(1, XS):
        grad = grad + vp[source].astype(F32)
    grad = grad * norm
    gv_ref[...] = grad
    score = jnp.sqrt(jnp.sum(grad * grad, axis=0, keepdims=True))
    score = jnp.where(active > 0.0, F32(0.0), score)
    score_ref[...] = score
    best = score[:, :128]
    for at in range(128, width, 128):
        best = jnp.maximum(best, score[:, at : at + 128])
    tops[2 * CHIPS - 2] = best

    def top_copy(i, which):
        slot = i * 2 + which
        target = to_chip(i) * 2 + (core if which == 0 else other)
        return send(
            tops.at[2 * CHIPS - 2],
            tops.at[slot],
            top_send.at[slot],
            top_recv.at[slot],
            target,
            samp,
        )

    def start_top(i, carry):
        top_copy(i, 0).start()
        top_copy(i, 1).start()
        return carry

    lax.fori_loop(0, CHIPS - 1, start_top, 0)
    top_copy(CHIPS - 1, 1).start()

    z_total = ring_sum(tr_z, z, tr_z_recv, along_z)
    gt_ref[...] = z_total

    to_pair.wait_send()

    def sent(i, carry):
        pred_copy(i).wait_send()
        w_copy(i).wait_send()
        relay_copy(i).wait_send()
        return carry

    lax.fori_loop(0, CHIPS - 1, sent, 0)
    relay_copy(CHIPS - 1).wait_send()
    tr_core_copy.wait_send()
    for copy in (*x_copies, *y_copies, *z_copies):
        copy.wait_send()
    for step in range(1, XS):
        vp_copy(step).wait_send()

    def top_wait(i, carry):
        for which in range(2):
            top_copy(i, which).wait()
        return carry

    lax.fori_loop(0, CHIPS - 1, top_wait, 0)
    top_copy(CHIPS - 1, 1).wait()
    top = jnp.max(tops[...], axis=0)
    top_ref[...] = jnp.max(top, axis=1, keepdims=True)


def per_device(genotypes, labels, act_coef, act_index, act_count, loadings, intercept):
    sample_rows, width = genotypes.shape
    rows, traits = labels.shape
    rank = loadings.shape[0]
    slots = act_index.shape[0]
    norm = 1.0 / math.sqrt(sample_rows * lax.axis_size("samp"))
    dma = pltpu.SemaphoreType.DMA
    hbm = pl.BlockSpec(memory_space=pl.ANY)
    vmem = pl.BlockSpec(memory_space=pltpu.VMEM)
    blocks = (CHIPS, rank, rows)
    trait = (rank, traits)
    grad_var, grad_trait, score, top = pl.pallas_call(
        functools.partial(kernel, norm),
        out_shape=(
            jax.ShapeDtypeStruct((rank, width), F32),
            jax.ShapeDtypeStruct(trait, F32),
            jax.ShapeDtypeStruct((1, width), F32),
            jax.ShapeDtypeStruct((1, 1), F32),
        ),
        in_specs=[hbm] * 7,
        out_specs=(vmem,) * 4,
        scratch_shapes=[
            pltpu.VMEM((2 * CHIPS, rows, width), BF16),
            pltpu.VMEM((rows, traits), jnp.int32),
            pltpu.VMEM((rank, slots), BF16),
            pltpu.VMEM((1, slots), jnp.int32),
            pltpu.VMEM((1, 1), jnp.int32),
            pltpu.VMEM(trait, F32),
            pltpu.VMEM((1, traits), F32),
            pltpu.VMEM(blocks, BF16),
            pltpu.VMEM(blocks, BF16),
            pltpu.VMEM(blocks, BF16),
            pltpu.VMEM(blocks, BF16),
            pltpu.VMEM(blocks, BF16),
            pltpu.VMEM(blocks, BF16),
            pltpu.VMEM((XS, rank, width), BF16),
            pltpu.VMEM((2 * CHIPS, 1, 128), F32),
            pltpu.VMEM(trait, F32),
            pltpu.VMEM(trait, F32),
            pltpu.VMEM((XS, *trait), F32),
            pltpu.VMEM((SIDE, *trait), F32),
            pltpu.VMEM((SIDE, *trait), F32),
            dma((2 * CHIPS,)),
            dma((6,)),
            dma,
            dma,
            dma((CHIPS,)),
            dma((CHIPS,)),
            dma((CHIPS,)),
            dma((CHIPS,)),
            dma((CHIPS,)),
            dma((CHIPS,)),
            dma((XS,)),
            dma((XS,)),
            dma((2 * CHIPS,)),
            dma((2 * CHIPS,)),
            dma((10,)),
            dma,
            dma((XS,)),
            dma((SIDE,)),
            dma((SIDE,)),
        ],
        compiler_params=pltpu.CompilerParams(collective_id=0, has_side_effects=True),
    )(
        genotypes,
        labels,
        act_coef,
        act_index.reshape(1, slots),
        act_count.reshape(1, 1),
        loadings,
        intercept.reshape(1, traits),
    )
    return grad_var, grad_trait, score.reshape(width), top.reshape(1)


def solution(mesh):
    placed = (
        P("samp", "var"),
        P(("samp", "var"), None),
        P(None, "var"),
        P("var"),
        P("var"),
        P(),
        P(),
    )
    return jax.shard_map(
        per_device,
        mesh=mesh,
        in_specs=placed,
        out_specs=(P(None, "var"), P(), P("var"), P()),
        check_vma=False,
    )
```

```python
import functools
import math

import jax
import jax.numpy as jnp
from jax import lax
from jax.experimental import pallas as pl
from jax.experimental.pallas import tpu as pltpu
from jax.sharding import PartitionSpec as P

MESH = pl.DeviceIdType.MESH
F32 = jnp.float32
BF16 = jnp.bfloat16
SIDE = 4
CHIPS = SIDE * SIDE
XS = 4
STEPS = sorted(
    ((a, b) for a in range(SIDE) for b in range(SIDE)),
    key=lambda s: -sum(min(k, SIDE - k) for k in s),
)
HERE = CHIPS - 1
EARLY = 10
NT = (((1,), (1,)), ((), ()))
TN = (((0,), (0,)), ((), ()))
NN = (((1,), (0,)), ((), ()))


def div(a, b):
    return lax.div(a, jnp.int32(b))


def rem(a, b):
    return lax.rem(a, jnp.int32(b))


def div(a, b):
    return lax.div(a, jnp.int32(b))


def rem(a, b):
    return lax.rem(a, jnp.int32(b))


def dot(a, b, dims):
    return lax.dot_general(a, b, dims, preferred_element_type=F32)


def halves(x):
    high = x.astype(BF16)
    return high, (x - high.astype(F32)).astype(BF16)


def kernel(
    norm, geno_hbm, labels_hbm, coef_hbm, index_hbm, count_ref, load_hbm, icpt_hbm,
    gv_ref, gt_ref, score_ref, top_ref,
    geno, labels, coef, index, load, icpt,
    pair_out, pair_in, own, pred_out, pred_in, w_same, w_pair, vp, tops,
    tr_own, tr_core, tr_x, tr_y, tr_z,
    geno_sem, small_sem, pair_send, pair_recv, pred_send, pred_recv,
    w_send, w_recv, relay_send, relay_recv, vp_send, vp_recv, top_send, top_recv,
    tr_send, tr_core_recv, tr_x_recv, tr_y_recv, tr_z_recv,
):
    me = lax.axis_index("var")
    samp = lax.axis_index("samp")
    core = rem(me, 2)
    chip = div(me, 2)
    y, z = div(chip, SIDE), rem(chip, SIDE)
    other = 1 - core
    partner = chip * 2 + other
    ys = [rem(y + k, SIDE) * SIDE for k in range(SIDE)]
    zs = [rem(z + k, SIDE) for k in range(SIDE)]
    xs = [rem(samp + k, XS) for k in range(XS)]
    to_chip = [(ys[a] + zs[b]) * 2 for a, b in STEPS]
    from_chip = [(ys[-a % SIDE] + zs[-b % SIDE]) * 2 for a, b in STEPS]

    def send(src, dst, send_sem, recv_sem, var, samp_at):
        return pltpu.make_async_remote_copy(
            src_ref=src,
            dst_ref=dst,
            send_sem=send_sem,
            recv_sem=recv_sem,
            device_id=(var, samp_at),
            device_id_type=MESH,
        )

    rows = labels.shape[0]

    def geno_copy(i, which):
        at = to_chip[i] + which
        return pltpu.make_async_copy(
            geno_hbm.at[pl.ds(pl.multiple_of(at * rows, rows), rows)], geno.at[at], geno_sem.at[at]
        )

    small = [
        pltpu.make_async_copy(src, dst, small_sem.at[k])
        for k, (src, dst) in enumerate(
            (
                (index_hbm, index),
                (coef_hbm, coef),
                (load_hbm, load),
                (icpt_hbm, icpt),
                (labels_hbm, labels),
            )
        )
    ]
    for copy in small[:2]:
        copy.start()
    for i in range(2):
        geno_copy(i, other).start()
    barrier = pltpu.get_barrier_semaphore()

    def greet(var, samp_at):
        pl.semaphore_signal(barrier, inc=1, device_id=(var, samp_at), device_id_type=MESH)

    for i in range(HERE):
        for which in range(2):
            greet(to_chip[i] + which, samp)
    for step in range(1, XS):
        greet(me, xs[step])
    greet(partner, samp)
    for i in range(2, CHIPS):
        geno_copy(i, other).start()
    for i in range(CHIPS):
        geno_copy(i, core).start()
    for copy in small[2:]:
        copy.start()

    for copy in small[:2]:
        copy.wait()
    slots = index.shape[1]
    width = geno.shape[2]
    live = lax.broadcasted_iota(jnp.int32, (1, slots), 1) < count_ref[0]
    variant = lax.broadcasted_iota(jnp.int32, (width, slots), 0)
    chosen = jnp.where((variant == index[...]) & live, F32(1.0), F32(0.0)).astype(BF16)
    dense = dot(coef[...], chosen, NT).astype(BF16)
    active = dot(jnp.where(live, F32(1.0), F32(0.0)).astype(BF16), chosen, NT)

    def partial(i, which):
        geno_copy(i, which).wait()
        return dot(dense, geno[to_chip[i] + which], NT)

    for i in range(CHIPS):
        pair_out[i] = partial(i, other).astype(BF16)
    pl.semaphore_wait(barrier, 2 * HERE + XS)

    half = CHIPS // 2
    to_pair = [
        send(
            pair_out.at[pl.ds(k * half, half)],
            pair_in.at[pl.ds(k * half, half)],
            pair_send.at[k],
            pair_recv.at[k],
            partner,
            samp,
        )
        for k in range(2)
    ]
    for copy in to_pair:
        copy.start()

    pred = [
        send(
            pred_out.at[i], pred_in.at[i], pred_send.at[i], pred_recv.at[i], to_chip[i] + core, samp
        )
        for i in range(HERE)
    ]

    def send_pred(i, part):
        pred_out[i] = (part + pair_in[i].astype(F32)).astype(BF16)
        pred[i].start()

    for i in range(EARLY):
        own[i] = partial(i, core)
    to_pair[0].wait_recv()
    for i in range(half):
        send_pred(i, own[i])
    to_pair[1].wait_recv()
    for i in range(half, EARLY):
        send_pred(i, own[i])
    for i in range(EARLY, HERE):
        send_pred(i, partial(i, core))
    mine = partial(HERE, core) + pair_in[HERE].astype(F32)

    for copy in small[2:]:
        copy.wait()
    load_h, load_m = halves(load[...])
    load_both = jnp.concatenate([load_h, load_m], axis=0)
    for i in reversed(range(HERE)):
        pred[i].wait_recv()
        mine = mine + pred_in[i].astype(F32)
    mine_h, mine_m = halves(mine)
    eta = (
        dot(
            jnp.concatenate([mine_h, mine_h, mine_m], axis=0),
            jnp.concatenate([load_h, load_m, load_h], axis=0),
            TN,
        )
        + icpt[...]
    )
    resid = 1.0 / (1.0 + jnp.exp(-eta)) - labels[...].astype(F32)
    resid_h, resid_m = halves(resid)
    first = dot(load_both, resid_h, NT)
    rank = load.shape[0]
    weights = first[:rank] + first[rank:] + dot(load_h, resid_m, NT)
    w_same[HERE] = weights.astype(BF16)

    to_same = [
        send(
            w_same.at[HERE], w_same.at[i], w_send.at[i], w_recv.at[i], to_chip[i] + core, samp
        )
        for i in range(HERE)
    ]
    relay = [
        send(w_same.at[i], w_pair.at[i], relay_send.at[i], relay_recv.at[i], partner, samp)
        for i in range(CHIPS)
    ]
    for copy in to_same:
        copy.start()
    relay[HERE].start()

    both = dot(jnp.concatenate([mine_h, mine_m], axis=0), resid_h, NN)
    tr_own[...] = (both[:rank] + both[rank:] + dot(mine_h, resid_m, NN)) * norm
    tr_core_copy = send(tr_own, tr_core, tr_send.at[0], tr_core_recv, partner, samp)
    tr_core_copy.start()

    def same_block(i, total):
        return total + dot(w_same[i], geno[from_chip[i] + core], NN)

    def pair_block(i, total):
        relay[i].wait_recv()
        return total + dot(w_pair[i], geno[from_chip[i] + other], NN)

    def arrived(i):
        to_same[i].wait_recv()
        relay[i].start()

    def ring_copies(slots, at, base, recv_sems, peers):
        return [
            send(
                slots.at[at], slots.at[at], tr_send.at[base + k], recv_sems.at[at], *peer
            )
            for k, peer in enumerate(peers)
        ]

    def ring_start(value, slots, at, base, recv_sems, peers):
        slots[at] = value
        copies = ring_copies(slots, at, base, recv_sems, peers)
        for copy in copies:
            copy.start()
        return copies

    def ring_sum(slots, sources, recv_sems, peer):
        for source in sources:
            send(
                slots.at[source], slots.at[source], tr_send.at[0], recv_sems.at[source], *peer
            ).wait_recv()
        return (slots[0] + slots[1]) + (slots[2] + slots[3])

    x_peers = [(me, xs[k]) for k in range(1, XS)]
    y_peers = [((ys[k] + z) * 2 + core, samp) for k in range(1, SIDE)]
    z_peers = [((y * SIDE + zs[k]) * 2 + core, samp) for k in range(1, SIDE)]
    y_at = [rem(y + k, SIDE) for k in range(1, SIDE)]

    total = same_block(HERE, jnp.zeros((rank, width), F32))
    for i in range(HERE - 1, 10, -1):
        arrived(i)
        total = same_block(i, total)
        total = pair_block(i + 1, total)
    tr_core_copy.wait_recv()
    x_copies = ring_start(tr_own[...] + tr_core[...], tr_x, samp, 1, tr_x_recv, x_peers)
    for i in range(10, 4, -1):
        arrived(i)
        total = same_block(i, total)
        total = pair_block(i + 1, total)
    for i in range(4, -1, -1):
        arrived(i)
        total = same_block(i, total)
    x_total = ring_sum(tr_x, xs[1:], tr_x_recv, x_peers[0])
    y_copies = ring_start(x_total, tr_y, y, 4, tr_y_recv, y_peers)
    for i in range(5, -1, -1):
        total = pair_block(i, total)

    vp[samp] = total.astype(BF16)
    to_x = [
        send(vp.at[samp], vp.at[samp], vp_send.at[k], vp_recv.at[samp], *peer)
        for k, peer in enumerate(x_peers)
    ]
    for copy in to_x:
        copy.start()
    y_total = ring_sum(tr_y, y_at, tr_y_recv, y_peers[0])
    z_copies = ring_start(y_total, tr_z, z, 7, tr_z_recv, z_peers)
    for source in xs[1:]:
        send(
            vp.at[source], vp.at[source], vp_send.at[0], vp_recv.at[source], *x_peers[0]
        ).wait_recv()
    grad = vp[0].astype(F32)
    for source in range(1, XS):
        grad = grad + vp[source].astype(F32)
    grad = grad * norm
    score = jnp.sqrt(jnp.sum(grad * grad, axis=0, keepdims=True))
    score = jnp.where(active > 0.0, F32(0.0), score)
    best = score[:, :128]
    for at in range(128, width, 128):
        best = jnp.maximum(best, score[:, at : at + 128])
    tops[2 * HERE] = best
    to_top = [
        send(
            tops.at[2 * HERE],
            tops.at[2 * i + k],
            top_send.at[2 * i + k],
            top_recv.at[2 * i + k],
            to_chip[i] + which,
            samp,
        )
        for i in range(CHIPS)
        for k, which in enumerate((core, other))
        if 2 * i + k != 2 * HERE
    ]
    for copy in to_top:
        copy.start()
    gv_ref[...] = grad
    score_ref[...] = score
    gt_ref[...] = ring_sum(tr_z, zs[1:], tr_z_recv, z_peers[0])

    for copy in (
        *to_pair, *pred, *to_same, *relay, tr_core_copy, *x_copies, *y_copies, *z_copies, *to_x, *to_top
    ):
        copy.wait_send()
    for copy in to_top:
        copy.wait_recv()
    top_ref[...] = jnp.broadcast_to(
        jnp.max(jnp.max(tops[...], axis=0), axis=1, keepdims=True), top_ref.shape
    )


def keep(*refs):
    *refs, sems = refs
    half = len(refs) // 2
    copies = [
        pltpu.make_async_copy(source, target, sems.at[k])
        for k, (source, target) in enumerate(zip(refs[:half], refs[half:]))
    ]
    for copy in copies:
        copy.start()
    for copy in copies:
        copy.wait()


def per_device(genotypes, labels, act_coef, act_index, act_count, loadings, intercept):
    sample_rows, width = genotypes.shape
    rows, traits = labels.shape
    rank = loadings.shape[0]
    slots = act_index.shape[0]
    norm = 1.0 / math.sqrt(sample_rows * lax.axis_size("samp"))
    dma = pltpu.SemaphoreType.DMA
    anywhere = pl.BlockSpec(memory_space=pl.ANY)
    vmem = pl.BlockSpec(memory_space=pltpu.VMEM)
    blocks = (CHIPS, rank, rows)
    trait = (rank, traits)
    in_hbm = functools.partial(pltpu.with_memory_space_constraint, memory_space=pltpu.HBM)
    results = pl.pallas_call(
        functools.partial(kernel, norm),
        out_shape=(
            jax.ShapeDtypeStruct((rank, width), F32),
            jax.ShapeDtypeStruct(trait, F32),
            jax.ShapeDtypeStruct((1, width), F32),
            jax.ShapeDtypeStruct((1, 128), F32),
        ),
        in_specs=[
            *(anywhere,) * 4,
            pl.BlockSpec(memory_space=pltpu.SMEM),
            *(anywhere,) * 2,
        ],
        out_specs=(vmem,) * 4,
        scratch_shapes=[
            pltpu.VMEM((2 * CHIPS, rows, width), BF16),
            pltpu.VMEM((rows, traits), jnp.int32),
            pltpu.VMEM((rank, slots), BF16),
            pltpu.VMEM((1, slots), jnp.int32),
            pltpu.VMEM(trait, F32),
            pltpu.VMEM((1, traits), F32),
            pltpu.VMEM(blocks, BF16),
            pltpu.VMEM(blocks, BF16),
            pltpu.VMEM((EARLY, rank, rows), F32),
            pltpu.VMEM(blocks, BF16),
            pltpu.VMEM(blocks, BF16),
            pltpu.VMEM(blocks, BF16),
            pltpu.VMEM(blocks, BF16),
            pltpu.VMEM((XS, rank, width), BF16),
            pltpu.VMEM((2 * CHIPS, 1, 128), F32),
            pltpu.VMEM(trait, F32),
            pltpu.VMEM(trait, F32),
            pltpu.VMEM((XS, *trait), F32),
            pltpu.VMEM((SIDE, *trait), F32),
            pltpu.VMEM((SIDE, *trait), F32),
            dma((2 * CHIPS,)),
            dma((5,)),
            dma((2,)),
            dma((2,)),
            dma((CHIPS,)),
            dma((CHIPS,)),
            dma((CHIPS,)),
            dma((CHIPS,)),
            dma((CHIPS,)),
            dma((CHIPS,)),
            dma((XS,)),
            dma((XS,)),
            dma((2 * CHIPS,)),
            dma((2 * CHIPS,)),
            dma((10,)),
            dma,
            dma((XS,)),
            dma((SIDE,)),
            dma((SIDE,)),
        ],
        compiler_params=pltpu.CompilerParams(
            collective_id=0, has_side_effects=True, vmem_limit_bytes=48 * 1024 * 1024
        ),
    )(
        in_hbm(genotypes),
        in_hbm(labels),
        in_hbm(act_coef),
        in_hbm(act_index.reshape(1, slots)),
        act_count,
        in_hbm(loadings),
        in_hbm(intercept.reshape(1, traits)),
    )
    grad_var, grad_trait, score, top = pl.pallas_call(
        keep,
        out_shape=tuple(jax.ShapeDtypeStruct(x.shape, x.dtype) for x in results),
        in_specs=[anywhere] * len(results),
        out_specs=(anywhere,) * len(results),
        scratch_shapes=[dma((len(results),))],
        compiler_params=pltpu.CompilerParams(vmem_limit_bytes=4 * 1024 * 1024),
    )(*results)
    return grad_var, grad_trait, score.reshape(width), top[0, :1]


def solution(mesh):
    placed = (
        P("samp", "var"),
        P(("samp", "var"), None),
        P(None, "var"),
        P("var"),
        P("var"),
        P(),
        P(),
    )
    return jax.shard_map(
        per_device,
        mesh=mesh,
        in_specs=placed,
        out_specs=(P(None, "var"), P(), P("var"), P()),
        check_vma=False,
    )
```

```python
import functools
import math

import jax
import jax.numpy as jnp
from jax import lax
from jax.experimental import pallas as pl
from jax.experimental.pallas import tpu as pltpu
from jax.sharding import PartitionSpec as P

MESH = pl.DeviceIdType.MESH
F32 = jnp.float32
BF16 = jnp.bfloat16
SIDE = 4
CHIPS = SIDE * SIDE
XS = 4
STEPS = sorted(
    ((a, b) for a in range(SIDE) for b in range(SIDE)),
    key=lambda s: -sum(min(k, SIDE - k) for k in s),
)
HERE = CHIPS - 1
BATCHES = ((0, 1), (2, 3), (4, 5), (6, 7, 8), (9, 10, 11), (12, 13), (14, 15))
BEFORE = 3
NEAR, MIDDLE, FAR = (15, 14, 13, 12, 11), (10, 9, 8, 7, 6, 5), (4, 3, 2, 1)
NT = (((1,), (1,)), ((), ()))
TN = (((0,), (0,)), ((), ()))
NN = (((1,), (0,)), ((), ()))


def div(a, b):
    return lax.div(a, jnp.int32(b))


def rem(a, b):
    return lax.rem(a, jnp.int32(b))


def div(a, b):
    return lax.div(a, jnp.int32(b))


def rem(a, b):
    return lax.rem(a, jnp.int32(b))


def dot(a, b, dims):
    return lax.dot_general(a, b, dims, preferred_element_type=F32)


def halves(x):
    high = x.astype(BF16)
    return high, (x - high.astype(F32)).astype(BF16)


def kernel(
    norm, geno_hbm, labels_hbm, coef_hbm, index_hbm, count_ref, load_hbm, icpt_hbm,
    gv_ref, gt_ref, score_ref, top_ref,
    geno, labels, coef, index, load, icpt,
    pred_out, pred_in, w_in, vp, tops,
    tr_own, tr_core, tr_x, tr_y, tr_z,
    geno_sem, small_sem, pred_send, pred_recv, w_send, w_recv, vp_send, vp_recv, top_send, top_recv,
    tr_send, tr_core_recv, tr_x_recv, tr_y_recv, tr_z_recv,
):
    me = lax.axis_index("var")
    samp = lax.axis_index("samp")
    core = rem(me, 2)
    chip = div(me, 2)
    y, z = div(chip, SIDE), rem(chip, SIDE)
    other = 1 - core
    partner = chip * 2 + other
    ys = [rem(y + k, SIDE) * SIDE for k in range(SIDE)]
    zs = [rem(z + k, SIDE) for k in range(SIDE)]
    xs = [rem(samp + k, XS) for k in range(XS)]
    to_chip = [ys[a] + zs[b] for a, b in STEPS]
    from_chip = [ys[-a % SIDE] + zs[-b % SIDE] for a, b in STEPS]

    def send(src, dst, send_sem, recv_sem, var, samp_at):
        return pltpu.make_async_remote_copy(
            src_ref=src,
            dst_ref=dst,
            send_sem=send_sem,
            recv_sem=recv_sem,
            device_id=(var, samp_at),
            device_id_type=MESH,
        )

    rows = labels.shape[0]

    def geno_copy(i):
        at = to_chip[i]
        return pltpu.make_async_copy(
            geno_hbm.at[pl.ds(pl.multiple_of(at * 2 * rows, 2 * rows), 2 * rows)],
            geno.at[at],
            geno_sem.at[i],
        )

    small = [
        pltpu.make_async_copy(src, dst, small_sem.at[k])
        for k, (src, dst) in enumerate(
            (
                (index_hbm, index),
                (coef_hbm, coef),
                (load_hbm, load),
                (icpt_hbm, icpt),
                (labels_hbm, labels),
            )
        )
    ]
    for copy in small[:2]:
        copy.start()
    for i in range(2):
        geno_copy(i).start()
    barrier = pltpu.get_barrier_semaphore()

    def greet(var, samp_at):
        pl.semaphore_signal(barrier, inc=1, device_id=(var, samp_at), device_id_type=MESH)

    for i in range(HERE):
        for which in range(2):
            greet(to_chip[i] * 2 + which, samp)
    for step in range(1, XS):
        greet(me, xs[step])
    greet(partner, samp)
    for i in range(2, CHIPS):
        geno_copy(i).start()
    for copy in small[2:]:
        copy.start()

    for copy in small[:2]:
        copy.wait()
    slots = index.shape[1]
    width = geno.shape[2]
    live = lax.broadcasted_iota(jnp.int32, (1, slots), 1) < count_ref[0]
    variant = lax.broadcasted_iota(jnp.int32, (width, slots), 0)
    chosen = jnp.where((variant == index[...]) & live, F32(1.0), F32(0.0)).astype(BF16)
    dense = dot(coef[...], chosen, NT).astype(BF16)
    active = dot(jnp.where(live, F32(1.0), F32(0.0)).astype(BF16), chosen, NT)

    def across(source, target, send_sem, recv_sem, i, which):
        return send(
            source,
            target.at[2 * i + core],
            send_sem.at[2 * i + which],
            recv_sem.at[2 * i + core],
            to_chip[i] * 2 + which,
            samp,
        )

    def landed(target, send_sem, recv_sem, i, which):
        send(
            target.at[2 * i + which],
            target.at[2 * i + which],
            send_sem.at[2 * i],
            recv_sem.at[2 * i + which],
            partner,
            samp,
        ).wait_recv()

    pred = [
        across(pred_out.at[2 * i + which], pred_in, pred_send, pred_recv, i, which)
        for i in range(HERE)
        for which in range(2)
    ]
    pred_pair = across(pred_out.at[2 * HERE], pred_in, pred_send, pred_recv, HERE, other)
    for n, batch in enumerate(BATCHES):
        for i in batch:
            geno_copy(i).wait()
        parts = [dot(dense, geno[to_chip[i]], NT) for i in batch]
        for i, part in zip(batch, parts):
            if i == HERE:
                mine = jnp.where(core == 0, part[:, :rows], part[:, rows:])
                pred_out[2 * HERE] = jnp.where(core == 0, part[:, rows:], part[:, :rows]).astype(BF16)
            else:
                for which in range(2):
                    pred_out[2 * i + which] = part[:, which * rows : (which + 1) * rows].astype(BF16)
        if n == BEFORE - 1:
            pl.semaphore_wait(barrier, 2 * HERE + XS)
        ready = [i for k in BATCHES[: n + 1] for i in k] if n == BEFORE - 1 else batch
        if n >= BEFORE - 1:
            for i in ready:
                if i == HERE:
                    pred_pair.start()
                else:
                    pred[2 * i].start()
                    pred[2 * i + 1].start()

    for copy in small[2:]:
        copy.wait()
    load_h, load_m = halves(load[...])
    load_both = jnp.concatenate([load_h, load_m], axis=0)
    for i in range(HERE):
        for which in range(2):
            landed(pred_in, pred_send, pred_recv, i, which)
        mine = mine + (pred_in[2 * i].astype(F32) + pred_in[2 * i + 1].astype(F32))
    landed(pred_in, pred_send, pred_recv, HERE, other)
    mine = mine + pred_in[2 * HERE + other].astype(F32)
    mine_h, mine_m = halves(mine)
    eta = (
        dot(
            jnp.concatenate([mine_h, mine_h, mine_m], axis=0),
            jnp.concatenate([load_h, load_m, load_h], axis=0),
            TN,
        )
        + icpt[...]
    )
    resid = 1.0 / (1.0 + jnp.exp(-eta)) - labels[...].astype(F32)
    resid_h, resid_m = halves(resid)
    first = dot(load_both, resid_h, NT)
    rank = load.shape[0]
    weights = first[:rank] + first[rank:] + dot(load_h, resid_m, NT)
    w_own = w_in.at[2 * HERE + core]
    w_own[...] = weights.astype(BF16)
    to_w = [across(w_own, w_in, w_send, w_recv, HERE, other)]
    for i in reversed(range(HERE)):
        for which in range(2):
            to_w.append(across(w_own, w_in, w_send, w_recv, i, which))
    for copy in to_w:
        copy.start()

    both = dot(jnp.concatenate([mine_h, mine_m], axis=0), resid_h, NN)
    tr_own[...] = (both[:rank] + both[rank:] + dot(mine_h, resid_m, NN)) * norm
    tr_core_copy = send(tr_own, tr_core, tr_send.at[0], tr_core_recv, partner, samp)
    tr_core_copy.start()

    def products(batch, total):
        for i in batch:
            for which in (other,) if i == HERE else (0, 1):
                landed(w_in, w_send, w_recv, i, which)
        for i in batch:
            both = jnp.concatenate([w_in[2 * i], w_in[2 * i + 1]], axis=1)
            part = dot(both, geno[from_chip[i]], NN)
            total = part if total is None else total + part
        return total

    def ring_copies(slots, at, base, recv_sems, peers):
        return [
            send(
                slots.at[at], slots.at[at], tr_send.at[base + k], recv_sems.at[at], *peer
            )
            for k, peer in enumerate(peers)
        ]

    def ring_start(value, slots, at, base, recv_sems, peers):
        slots[at] = value
        copies = ring_copies(slots, at, base, recv_sems, peers)
        for copy in copies:
            copy.start()
        return copies

    def ring_sum(slots, sources, recv_sems, peer):
        for source in sources:
            send(
                slots.at[source], slots.at[source], tr_send.at[0], recv_sems.at[source], *peer
            ).wait_recv()
        return (slots[0] + slots[1]) + (slots[2] + slots[3])

    x_peers = [(me, xs[k]) for k in range(1, XS)]
    y_peers = [((ys[k] + z) * 2 + core, samp) for k in range(1, SIDE)]
    z_peers = [((y * SIDE + zs[k]) * 2 + core, samp) for k in range(1, SIDE)]
    y_at = [rem(y + k, SIDE) for k in range(1, SIDE)]

    total = products(NEAR, None)
    tr_core_copy.wait_recv()
    x_copies = ring_start(tr_own[...] + tr_core[...], tr_x, samp, 1, tr_x_recv, x_peers)
    total = products(MIDDLE, total)
    total = products(FAR, total)
    x_total = ring_sum(tr_x, xs[1:], tr_x_recv, x_peers[0])
    y_copies = ring_start(x_total, tr_y, y, 4, tr_y_recv, y_peers)
    total = products((0,), total)

    vp[samp] = total.astype(BF16)
    to_x = [
        send(vp.at[samp], vp.at[samp], vp_send.at[k], vp_recv.at[samp], *peer)
        for k, peer in enumerate(x_peers)
    ]
    for copy in to_x:
        copy.start()
    y_total = ring_sum(tr_y, y_at, tr_y_recv, y_peers[0])
    z_copies = ring_start(y_total, tr_z, z, 7, tr_z_recv, z_peers)
    for source in xs[1:]:
        send(
            vp.at[source], vp.at[source], vp_send.at[0], vp_recv.at[source], *x_peers[0]
        ).wait_recv()
    grad = vp[0].astype(F32)
    for source in range(1, XS):
        grad = grad + vp[source].astype(F32)
    grad = grad * norm
    score = jnp.sqrt(jnp.sum(grad * grad, axis=0, keepdims=True))
    score = jnp.where(active > 0.0, F32(0.0), score)
    best = score[:, :128]
    for at in range(128, width, 128):
        best = jnp.maximum(best, score[:, at : at + 128])
    tops[2 * HERE] = best
    to_top = [
        send(
            tops.at[2 * HERE],
            tops.at[2 * i + k],
            top_send.at[2 * i + k],
            top_recv.at[2 * i + k],
            to_chip[i] * 2 + which,
            samp,
        )
        for i in range(CHIPS)
        for k, which in enumerate((core, other))
        if 2 * i + k != 2 * HERE
    ]
    for copy in to_top:
        copy.start()
    gv_ref[...] = grad
    score_ref[...] = score
    gt_ref[...] = ring_sum(tr_z, zs[1:], tr_z_recv, z_peers[0])

    for copy in (
        *pred, pred_pair, *to_w, tr_core_copy, *x_copies, *y_copies, *z_copies, *to_x, *to_top
    ):
        copy.wait_send()
    for copy in to_top:
        copy.wait_recv()
    top_ref[...] = jnp.broadcast_to(
        jnp.max(jnp.max(tops[...], axis=0), axis=1, keepdims=True), top_ref.shape
    )


def keep(*refs):
    *refs, sems = refs
    half = len(refs) // 2
    copies = [
        pltpu.make_async_copy(source, target, sems.at[k])
        for k, (source, target) in enumerate(zip(refs[:half], refs[half:]))
    ]
    for copy in copies:
        copy.start()
    for copy in copies:
        copy.wait()


def per_device(genotypes, labels, act_coef, act_index, act_count, loadings, intercept):
    sample_rows, width = genotypes.shape
    rows, traits = labels.shape
    rank = loadings.shape[0]
    slots = act_index.shape[0]
    norm = 1.0 / math.sqrt(sample_rows * lax.axis_size("samp"))
    dma = pltpu.SemaphoreType.DMA
    anywhere = pl.BlockSpec(memory_space=pl.ANY)
    vmem = pl.BlockSpec(memory_space=pltpu.VMEM)
    blocks = (2 * CHIPS, rank, rows)
    trait = (rank, traits)
    in_hbm = functools.partial(pltpu.with_memory_space_constraint, memory_space=pltpu.HBM)
    results = pl.pallas_call(
        functools.partial(kernel, norm),
        out_shape=(
            jax.ShapeDtypeStruct((rank, width), F32),
            jax.ShapeDtypeStruct(trait, F32),
            jax.ShapeDtypeStruct((1, width), F32),
            jax.ShapeDtypeStruct((1, 128), F32),
        ),
        in_specs=[
            *(anywhere,) * 4,
            pl.BlockSpec(memory_space=pltpu.SMEM),
            *(anywhere,) * 2,
        ],
        out_specs=(vmem,) * 4,
        scratch_shapes=[
            pltpu.VMEM((CHIPS, 2 * rows, width), BF16),
            pltpu.VMEM((rows, traits), jnp.int32),
            pltpu.VMEM((rank, slots), BF16),
            pltpu.VMEM((1, slots), jnp.int32),
            pltpu.VMEM(trait, F32),
            pltpu.VMEM((1, traits), F32),
            pltpu.VMEM(blocks, BF16),
            pltpu.VMEM(blocks, BF16),
            pltpu.VMEM(blocks, BF16),
            pltpu.VMEM((XS, rank, width), BF16),
            pltpu.VMEM((2 * CHIPS, 1, 128), F32),
            pltpu.VMEM(trait, F32),
            pltpu.VMEM(trait, F32),
            pltpu.VMEM((XS, *trait), F32),
            pltpu.VMEM((SIDE, *trait), F32),
            pltpu.VMEM((SIDE, *trait), F32),
            dma((CHIPS,)),
            dma((5,)),
            dma((2 * CHIPS,)),
            dma((2 * CHIPS,)),
            dma((2 * CHIPS,)),
            dma((2 * CHIPS,)),
            dma((XS,)),
            dma((XS,)),
            dma((2 * CHIPS,)),
            dma((2 * CHIPS,)),
            dma((10,)),
            dma,
            dma((XS,)),
            dma((SIDE,)),
            dma((SIDE,)),
        ],
        compiler_params=pltpu.CompilerParams(
            collective_id=0, has_side_effects=True, vmem_limit_bytes=48 * 1024 * 1024
        ),
    )(
        in_hbm(genotypes),
        in_hbm(labels),
        in_hbm(act_coef),
        in_hbm(act_index.reshape(1, slots)),
        act_count,
        in_hbm(loadings),
        in_hbm(intercept.reshape(1, traits)),
    )
    grad_var, grad_trait, score, top = pl.pallas_call(
        keep,
        out_shape=tuple(jax.ShapeDtypeStruct(x.shape, x.dtype) for x in results),
        in_specs=[anywhere] * len(results),
        out_specs=(anywhere,) * len(results),
        scratch_shapes=[dma((len(results),))],
        compiler_params=pltpu.CompilerParams(vmem_limit_bytes=4 * 1024 * 1024),
    )(*results)
    return grad_var, grad_trait, score.reshape(width), top[0, :1]


def solution(mesh):
    placed = (
        P("samp", "var"),
        P(("samp", "var"), None),
        P(None, "var"),
        P("var"),
        P("var"),
        P(),
        P(),
    )
    return jax.shard_map(
        per_device,
        mesh=mesh,
        in_specs=placed,
        out_specs=(P(None, "var"), P(), P("var"), P()),
        check_vma=False,
    )
```

```python
import functools
import math

import jax
import jax.numpy as jnp
from jax import lax
from jax.experimental import pallas as pl
from jax.experimental.pallas import tpu as pltpu
from jax.sharding import PartitionSpec as P

MESH = pl.DeviceIdType.MESH
F32 = jnp.float32
BF16 = jnp.bfloat16
SIDE = 4
CHIPS = SIDE * SIDE
XS = 4
STEPS = sorted(
    ((a, b) for a in range(SIDE) for b in range(SIDE)),
    key=lambda s: -sum(min(k, SIDE - k) for k in s),
)
HERE = CHIPS - 1
BATCHES = ((0, 1), (2, 3), (4, 5), (6, 7, 8), (9, 10, 11), (12, 13), (14, 15))
BEFORE = 3
GROUPS = ((15, 14, 13, 12, 11), (10, 9, 8, 7, 6, 5), (4, 3, 2, 1), (0,))
NT = (((1,), (1,)), ((), ()))
TN = (((0,), (0,)), ((), ()))
NN = (((1,), (0,)), ((), ()))


def div(a, b):
    return lax.div(a, jnp.int32(b))


def rem(a, b):
    return lax.rem(a, jnp.int32(b))


def div(a, b):
    return lax.div(a, jnp.int32(b))


def rem(a, b):
    return lax.rem(a, jnp.int32(b))


def dot(a, b, dims):
    return lax.dot_general(a, b, dims, preferred_element_type=F32)


def halves(x):
    high = x.astype(BF16)
    return high, (x - high.astype(F32)).astype(BF16)


def kernel(
    norm, geno_hbm, labels_hbm, coef_hbm, index_hbm, count_ref, load_hbm, icpt_hbm,
    gv_ref, gt_ref, score_ref, top_ref,
    geno, labels, coef, index, load, icpt,
    pred_out, pred_in, w_in, vp, tops,
    tr_own, tr_core, tr_x, tr_y, tr_z,
    geno_sem, small_sem, pred_send, pred_recv, w_send, w_recv, vp_send, vp_recv, top_send, top_recv,
    tr_send, tr_recv,
):
    me = lax.axis_index("var")
    samp = lax.axis_index("samp")
    core = rem(me, 2)
    chip = div(me, 2)
    y, z = div(chip, SIDE), rem(chip, SIDE)
    other = 1 - core
    partner = chip * 2 + other
    ys = [rem(y + k, SIDE) * SIDE for k in range(SIDE)]
    zs = [rem(z + k, SIDE) for k in range(SIDE)]
    xs = [rem(samp + k, XS) for k in range(XS)]
    to_chip = [ys[a] + zs[b] for a, b in STEPS]
    from_chip = [ys[-a % SIDE] + zs[-b % SIDE] for a, b in STEPS]

    def send(src, dst, send_sem, recv_sem, var, samp_at):
        return pltpu.make_async_remote_copy(
            src_ref=src,
            dst_ref=dst,
            send_sem=send_sem,
            recv_sem=recv_sem,
            device_id=(var, samp_at),
            device_id_type=MESH,
        )

    rows = labels.shape[0]

    def geno_copy(i):
        at = to_chip[i]
        return pltpu.make_async_copy(
            geno_hbm.at[pl.ds(pl.multiple_of(at * 2 * rows, 2 * rows), 2 * rows)],
            geno.at[at],
            geno_sem.at[next(n for n, batch in enumerate(BATCHES) if i in batch)],
        )

    small = [
        pltpu.make_async_copy(src, dst, small_sem.at[k])
        for k, (src, dst) in enumerate(
            (
                (index_hbm, index),
                (coef_hbm, coef),
                (load_hbm, load),
                (icpt_hbm, icpt),
                (labels_hbm, labels),
            )
        )
    ]
    for copy in small[:2]:
        copy.start()
    for i in range(2):
        geno_copy(i).start()
    barrier = pltpu.get_barrier_semaphore()

    def greet(var, samp_at):
        pl.semaphore_signal(barrier, inc=1, device_id=(var, samp_at), device_id_type=MESH)

    for i in range(HERE):
        for which in range(2):
            greet(to_chip[i] * 2 + which, samp)
    for step in range(1, XS):
        greet(me, xs[step])
    greet(partner, samp)
    for i in range(2, CHIPS):
        geno_copy(i).start()
    for copy in small[2:]:
        copy.start()

    for copy in small[:2]:
        copy.wait()
    slots = index.shape[1]
    width = geno.shape[2]
    live = lax.broadcasted_iota(jnp.int32, (1, slots), 1) < count_ref[0]
    variant = lax.broadcasted_iota(jnp.int32, (width, slots), 0)
    chosen = jnp.where((variant == index[...]) & live, F32(1.0), F32(0.0)).astype(BF16)
    dense = dot(coef[...], chosen, NT).astype(BF16)
    active = dot(jnp.where(live, F32(1.0), F32(0.0)).astype(BF16), chosen, NT)

    def across(source, target, send_sem, recv_sem, i, which):
        return send(
            source, target.at[2 * i + core], send_sem, recv_sem, to_chip[i] * 2 + which, samp
        )

    def bytes_of(blocks, sem):
        return send(blocks, blocks, sem, sem, partner, samp)

    pred = [
        across(pred_out.at[2 * i + which], pred_in, pred_send, pred_recv, i, which)
        for i in range(HERE)
        for which in range(2)
    ]
    pred_pair = across(pred_out.at[2 * HERE], pred_in, pred_send, pred_recv, HERE, other)
    for n, batch in enumerate(BATCHES):
        whole = geno.at[pl.ds(0, len(batch))]
        pltpu.make_async_copy(whole, whole, geno_sem.at[n]).wait()
        parts = [dot(dense, geno[to_chip[i]], NT) for i in batch]
        for i, part in zip(batch, parts):
            if i == HERE:
                mine = jnp.where(core == 0, part[:, :rows], part[:, rows:])
                pred_out[2 * HERE] = jnp.where(core == 0, part[:, rows:], part[:, :rows]).astype(BF16)
            else:
                for which in range(2):
                    pred_out[2 * i + which] = part[:, which * rows : (which + 1) * rows].astype(BF16)
        if n == BEFORE - 1:
            pl.semaphore_wait(barrier, 2 * HERE + XS)
        ready = [i for k in BATCHES[: n + 1] for i in k] if n == BEFORE - 1 else batch
        if n >= BEFORE - 1:
            for i in ready:
                if i == HERE:
                    pred_pair.start()
                else:
                    pred[2 * i].start()
                    pred[2 * i + 1].start()

    for copy in small[2:]:
        copy.wait()
    load_h, load_m = halves(load[...])
    load_both = jnp.concatenate([load_h, load_m], axis=0)
    bytes_of(pred_in.at[pl.ds(0, 2 * HERE + 1)], pred_recv).wait_recv()
    for i in range(HERE):
        mine = mine + (pred_in[2 * i].astype(F32) + pred_in[2 * i + 1].astype(F32))
    mine = mine + pred_in[2 * HERE + other].astype(F32)
    mine_h, mine_m = halves(mine)
    eta = (
        dot(
            jnp.concatenate([mine_h, mine_h, mine_m], axis=0),
            jnp.concatenate([load_h, load_m, load_h], axis=0),
            TN,
        )
        + icpt[...]
    )
    resid = 1.0 / (1.0 + jnp.exp(-eta)) - labels[...].astype(F32)
    resid_h, resid_m = halves(resid)
    first = dot(load_both, resid_h, NT)
    rank = load.shape[0]
    weights = first[:rank] + first[rank:] + dot(load_h, resid_m, NT)
    w_own = w_in.at[2 * HERE + core]
    w_own[...] = weights.astype(BF16)
    to_w = [across(w_own, w_in, w_send, w_recv.at[0], HERE, other)]
    for i in reversed(range(HERE)):
        for which in range(2):
            group = next(n for n, batch in enumerate(GROUPS) if i in batch)
            to_w.append(across(w_own, w_in, w_send, w_recv.at[group], i, which))
    for copy in to_w:
        copy.start()

    both = dot(jnp.concatenate([mine_h, mine_m], axis=0), resid_h, NN)
    tr_own[...] = (both[:rank] + both[rank:] + dot(mine_h, resid_m, NN)) * norm
    tr_core_copy = send(tr_own, tr_core, tr_send.at[0], tr_recv.at[0], partner, samp)
    tr_core_copy.start()

    def products(group, total):
        batch = GROUPS[group]
        arriving = 2 * len(batch) - (1 if HERE in batch else 0)
        bytes_of(w_in.at[pl.ds(0, arriving)], w_recv.at[group]).wait_recv()
        for i in batch:
            both = jnp.concatenate([w_in[2 * i], w_in[2 * i + 1]], axis=1)
            part = dot(both, geno[from_chip[i]], NN)
            total = part if total is None else total + part
        return total

    def ring_start(value, slots, at, send_sem, recv_sem, peers):
        slots[at] = value
        for peer in peers:
            send(slots.at[at], slots.at[at], send_sem, recv_sem, *peer).start()

    def ring_sum(slots, recv_sem):
        bytes_of(slots.at[pl.ds(0, SIDE - 1)], recv_sem).wait_recv()
        return (slots[0] + slots[1]) + (slots[2] + slots[3])

    x_peers = [(me, xs[k]) for k in range(1, XS)]
    y_peers = [((ys[k] + z) * 2 + core, samp) for k in range(1, SIDE)]
    z_peers = [((y * SIDE + zs[k]) * 2 + core, samp) for k in range(1, SIDE)]

    total = products(0, None)
    tr_core_copy.wait_recv()
    ring_start(tr_own[...] + tr_core[...], tr_x, samp, tr_send.at[1], tr_recv.at[1], x_peers)
    for group in range(1, len(GROUPS)):
        total = products(group, total)

    vp[samp] = total.astype(BF16)
    for peer in x_peers:
        send(vp.at[samp], vp.at[samp], vp_send, vp_recv, *peer).start()
    ring_start(ring_sum(tr_x, tr_recv.at[1]), tr_y, y, tr_send.at[2], tr_recv.at[2], y_peers)
    ring_start(ring_sum(tr_y, tr_recv.at[2]), tr_z, z, tr_send.at[3], tr_recv.at[3], z_peers)
    bytes_of(vp.at[pl.ds(0, XS - 1)], vp_recv).wait_recv()
    grad = vp[0].astype(F32)
    for source in range(1, XS):
        grad = grad + vp[source].astype(F32)
    grad = grad * norm
    score = jnp.sqrt(jnp.sum(grad * grad, axis=0, keepdims=True))
    score = jnp.where(active > 0.0, F32(0.0), score)
    best = score[:, :128]
    for at in range(128, width, 128):
        best = jnp.maximum(best, score[:, at : at + 128])
    tops[2 * HERE + core] = best
    top_own = tops.at[2 * HERE + core]
    for i in range(HERE):
        for which in range(2):
            across(top_own, tops, top_send, top_recv, i, which).start()
    across(top_own, tops, top_send, top_recv, HERE, other).start()
    gv_ref[...] = grad
    score_ref[...] = score
    gt_ref[...] = ring_sum(tr_z, tr_recv.at[3])

    bytes_of(pred_in.at[pl.ds(0, 2 * HERE + 1)], pred_send).wait_send()
    bytes_of(w_in.at[pl.ds(0, 2 * HERE + 1)], w_send).wait_send()
    tr_core_copy.wait_send()
    for k, slots in ((1, tr_x), (2, tr_y), (3, tr_z)):
        bytes_of(slots.at[pl.ds(0, SIDE - 1)], tr_send.at[k]).wait_send()
    bytes_of(vp.at[pl.ds(0, XS - 1)], vp_send).wait_send()
    bytes_of(tops.at[pl.ds(0, 2 * HERE + 1)], top_send).wait_send()
    bytes_of(tops.at[pl.ds(0, 2 * HERE + 1)], top_recv).wait_recv()
    top_ref[...] = jnp.broadcast_to(
        jnp.max(jnp.max(tops[...], axis=0), axis=1, keepdims=True), top_ref.shape
    )


def keep(*refs):
    *refs, sems = refs
    half = len(refs) // 2
    copies = [
        pltpu.make_async_copy(source, target, sems.at[k])
        for k, (source, target) in enumerate(zip(refs[:half], refs[half:]))
    ]
    for copy in copies:
        copy.start()
    for copy in copies:
        copy.wait()


def per_device(genotypes, labels, act_coef, act_index, act_count, loadings, intercept):
    sample_rows, width = genotypes.shape
    rows, traits = labels.shape
    rank = loadings.shape[0]
    slots = act_index.shape[0]
    norm = 1.0 / math.sqrt(sample_rows * lax.axis_size("samp"))
    dma = pltpu.SemaphoreType.DMA
    anywhere = pl.BlockSpec(memory_space=pl.ANY)
    vmem = pl.BlockSpec(memory_space=pltpu.VMEM)
    blocks = (2 * CHIPS, rank, rows)
    trait = (rank, traits)
    in_hbm = functools.partial(pltpu.with_memory_space_constraint, memory_space=pltpu.HBM)
    results = pl.pallas_call(
        functools.partial(kernel, norm),
        out_shape=(
            jax.ShapeDtypeStruct((rank, width), F32),
            jax.ShapeDtypeStruct(trait, F32),
            jax.ShapeDtypeStruct((1, width), F32),
            jax.ShapeDtypeStruct((1, 128), F32),
        ),
        in_specs=[
            *(anywhere,) * 4,
            pl.BlockSpec(memory_space=pltpu.SMEM),
            *(anywhere,) * 2,
        ],
        out_specs=(vmem,) * 4,
        scratch_shapes=[
            pltpu.VMEM((CHIPS, 2 * rows, width), BF16),
            pltpu.VMEM((rows, traits), jnp.int32),
            pltpu.VMEM((rank, slots), BF16),
            pltpu.VMEM((1, slots), jnp.int32),
            pltpu.VMEM(trait, F32),
            pltpu.VMEM((1, traits), F32),
            pltpu.VMEM(blocks, BF16),
            pltpu.VMEM(blocks, BF16),
            pltpu.VMEM(blocks, BF16),
            pltpu.VMEM((XS, rank, width), BF16),
            pltpu.VMEM((2 * CHIPS, 1, 128), F32),
            pltpu.VMEM(trait, F32),
            pltpu.VMEM(trait, F32),
            pltpu.VMEM((XS, *trait), F32),
            pltpu.VMEM((SIDE, *trait), F32),
            pltpu.VMEM((SIDE, *trait), F32),
            dma((len(BATCHES),)),
            dma((5,)),
            dma,
            dma,
            dma,
            dma((len(GROUPS),)),
            dma,
            dma,
            dma,
            dma,
            dma((4,)),
            dma((4,)),
        ],
        compiler_params=pltpu.CompilerParams(
            collective_id=0, has_side_effects=True, vmem_limit_bytes=48 * 1024 * 1024
        ),
    )(
        in_hbm(genotypes),
        in_hbm(labels),
        in_hbm(act_coef),
        in_hbm(act_index.reshape(1, slots)),
        act_count,
        in_hbm(loadings),
        in_hbm(intercept.reshape(1, traits)),
    )
    grad_var, grad_trait, score, top = pl.pallas_call(
        keep,
        out_shape=tuple(jax.ShapeDtypeStruct(x.shape, x.dtype) for x in results),
        in_specs=[anywhere] * len(results),
        out_specs=(anywhere,) * len(results),
        scratch_shapes=[dma((len(results),))],
        compiler_params=pltpu.CompilerParams(vmem_limit_bytes=4 * 1024 * 1024),
    )(*results)
    return grad_var, grad_trait, score.reshape(width), top[0, :1]


def solution(mesh):
    placed = (
        P("samp", "var"),
        P(("samp", "var"), None),
        P(None, "var"),
        P("var"),
        P("var"),
        P(),
        P(),
    )
    return jax.shard_map(
        per_device,
        mesh=mesh,
        in_specs=placed,
        out_specs=(P(None, "var"), P(), P("var"), P()),
        check_vma=False,
    )
```

```python
import functools
import math

import jax
import jax.numpy as jnp
from jax import lax
from jax.experimental import pallas as pl
from jax.experimental.pallas import tpu as pltpu
from jax.sharding import PartitionSpec as P

MESH = pl.DeviceIdType.MESH
F32 = jnp.float32
BF16 = jnp.bfloat16
SIDE = 4
CHIPS = SIDE * SIDE
XS = 4
STEPS = sorted(
    ((a, b) for a in range(SIDE) for b in range(SIDE)),
    key=lambda s: -sum(min(k, SIDE - k) for k in s),
)
HERE = CHIPS - 1
BATCHES = ((0, 1), (2, 3), (4, 5), (6, 7, 8), (9, 10, 11), (12, 13), (14, 15))
BEFORE = 3
GROUPS = ((15, 14, 13, 12, 11), (10, 9, 8, 7, 6, 5), (4, 3, 2, 1), (0,))
NT = (((1,), (1,)), ((), ()))
TN = (((0,), (0,)), ((), ()))
NN = (((1,), (0,)), ((), ()))


def div(a, b):
    return lax.div(a, jnp.int32(b))


def rem(a, b):
    return lax.rem(a, jnp.int32(b))


def div(a, b):
    return lax.div(a, jnp.int32(b))


def rem(a, b):
    return lax.rem(a, jnp.int32(b))


def dot(a, b, dims):
    return lax.dot_general(a, b, dims, preferred_element_type=F32)


def halves(x):
    high = x.astype(BF16)
    return high, (x - high.astype(F32)).astype(BF16)


def kernel(
    norm, geno_hbm, labels_hbm, coef_hbm, index_hbm, count_ref, load_hbm, icpt_hbm,
    gv_ref, gt_ref, score_ref, top_ref,
    geno, labels, coef, index, load, icpt,
    pred_out, pred_in, w_in, vp, tops,
    tr_own, tr_core, tr_x, tr_y, tr_z,
    geno_sem, small_sem, pred_send, pred_recv, w_send, w_recv, vp_send, vp_recv, top_send, top_recv,
    tr_send, tr_recv,
):
    me = lax.axis_index("var")
    samp = lax.axis_index("samp")
    core = rem(me, 2)
    chip = div(me, 2)
    y, z = div(chip, SIDE), rem(chip, SIDE)
    other = 1 - core
    partner = chip * 2 + other
    ys = [rem(y + k, SIDE) * SIDE for k in range(SIDE)]
    zs = [rem(z + k, SIDE) for k in range(SIDE)]
    xs = [rem(samp + k, XS) for k in range(XS)]
    to_chip = [ys[a] + zs[b] for a, b in STEPS]
    from_chip = [ys[-a % SIDE] + zs[-b % SIDE] for a, b in STEPS]

    def send(src, dst, send_sem, recv_sem, var, samp_at):
        return pltpu.make_async_remote_copy(
            src_ref=src,
            dst_ref=dst,
            send_sem=send_sem,
            recv_sem=recv_sem,
            device_id=(var, samp_at),
            device_id_type=MESH,
        )

    rows = labels.shape[0]

    def geno_copy(i):
        at = to_chip[i]
        return pltpu.make_async_copy(
            geno_hbm.at[pl.ds(pl.multiple_of(at * 2 * rows, 2 * rows), 2 * rows)],
            geno.at[at],
            geno_sem.at[next(n for n, batch in enumerate(BATCHES) if i in batch)],
        )

    small = [
        pltpu.make_async_copy(src, dst, small_sem.at[k])
        for k, (src, dst) in enumerate(
            (
                (index_hbm, index),
                (coef_hbm, coef),
                (load_hbm, load),
                (icpt_hbm, icpt),
                (labels_hbm, labels),
            )
        )
    ]
    for copy in small[:2]:
        copy.start()
    for i in range(2):
        geno_copy(i).start()
    barrier = pltpu.get_barrier_semaphore()

    def greet(var, samp_at):
        pl.semaphore_signal(barrier, inc=1, device_id=(var, samp_at), device_id_type=MESH)

    for i in range(HERE):
        for which in range(2):
            greet(to_chip[i] * 2 + which, samp)
    for step in range(1, XS):
        greet(me, xs[step])
    greet(partner, samp)
    for i in range(2, CHIPS):
        geno_copy(i).start()
    for copy in small[2:]:
        copy.start()

    for copy in small[:2]:
        copy.wait()
    slots = index.shape[1]
    width = geno.shape[2]
    live = lax.broadcasted_iota(jnp.int32, (1, slots), 1) < count_ref[0]
    variant = lax.broadcasted_iota(jnp.int32, (width, slots), 0)
    chosen = jnp.where((variant == index[...]) & live, F32(1.0), F32(0.0)).astype(BF16)
    dense = dot(coef[...], chosen, NT).astype(BF16)
    active = dot(jnp.where(live, F32(1.0), F32(0.0)).astype(BF16), chosen, NT)

    def across(source, target, send_sem, recv_sem, i, which):
        return send(
            source, target.at[2 * i + core], send_sem, recv_sem, to_chip[i] * 2 + which, samp
        )

    def bytes_of(blocks, sem):
        return send(blocks, blocks, sem, sem, partner, samp)

    pred = [
        across(pred_out.at[2 * i + which], pred_in, pred_send, pred_recv, i, which)
        for i in range(HERE)
        for which in range(2)
    ]
    pred_pair = across(pred_out.at[2 * HERE], pred_in, pred_send, pred_recv, HERE, other)
    for n, batch in enumerate(BATCHES):
        whole = geno.at[pl.ds(0, len(batch))]
        pltpu.make_async_copy(whole, whole, geno_sem.at[n]).wait()
        parts = [dot(dense, geno[to_chip[i]], NT) for i in batch]
        for i, part in zip(batch, parts):
            if i == HERE:
                mine = jnp.where(core == 0, part[:, :rows], part[:, rows:])
                pred_out[2 * HERE] = jnp.where(core == 0, part[:, rows:], part[:, :rows]).astype(BF16)
            else:
                for which in range(2):
                    pred_out[2 * i + which] = part[:, which * rows : (which + 1) * rows].astype(BF16)
        if n == BEFORE - 1:
            pl.semaphore_wait(barrier, 2 * HERE + XS)
        ready = [i for k in BATCHES[: n + 1] for i in k] if n == BEFORE - 1 else batch
        if n >= BEFORE - 1:
            for which in range(2):
                for i in ready:
                    if i != HERE:
                        pred[2 * i + which].start()
            if HERE in ready:
                pred_pair.start()

    for copy in small[2:]:
        copy.wait()
    load_h, load_m = halves(load[...])
    load_both = jnp.concatenate([load_h, load_m], axis=0)
    bytes_of(pred_in.at[pl.ds(0, 2 * HERE + 1)], pred_recv).wait_recv()
    for i in range(HERE):
        mine = mine + (pred_in[2 * i].astype(F32) + pred_in[2 * i + 1].astype(F32))
    mine = mine + pred_in[2 * HERE + other].astype(F32)
    mine_h, mine_m = halves(mine)
    eta = (
        dot(
            jnp.concatenate([mine_h, mine_h, mine_m], axis=0),
            jnp.concatenate([load_h, load_m, load_h], axis=0),
            TN,
        )
        + icpt[...]
    )
    resid = 1.0 / (1.0 + jnp.exp(-eta)) - labels[...].astype(F32)
    resid_h, resid_m = halves(resid)
    first = dot(load_both, resid_h, NT)
    rank = load.shape[0]
    weights = first[:rank] + first[rank:] + dot(load_h, resid_m, NT)
    w_own = w_in.at[2 * HERE + core]
    w_own[...] = weights.astype(BF16)
    to_w = [across(w_own, w_in, w_send, w_recv.at[0], HERE, other)]
    for group, batch in enumerate(GROUPS):
        for which in range(2):
            for i in batch:
                if i != HERE:
                    to_w.append(across(w_own, w_in, w_send, w_recv.at[group], i, which))
    for copy in to_w:
        copy.start()

    both = dot(jnp.concatenate([mine_h, mine_m], axis=0), resid_h, NN)
    tr_own[...] = (both[:rank] + both[rank:] + dot(mine_h, resid_m, NN)) * norm
    tr_core_copy = send(tr_own, tr_core, tr_send.at[0], tr_recv.at[0], partner, samp)
    tr_core_copy.start()

    def products(group, total):
        batch = GROUPS[group]
        arriving = 2 * len(batch) - (1 if HERE in batch else 0)
        bytes_of(w_in.at[pl.ds(0, arriving)], w_recv.at[group]).wait_recv()
        for i in batch:
            both = jnp.concatenate([w_in[2 * i], w_in[2 * i + 1]], axis=1)
            part = dot(both, geno[from_chip[i]], NN)
            total = part if total is None else total + part
        return total

    def ring_start(value, slots, at, send_sem, recv_sem, peers):
        slots[at] = value
        for peer in peers:
            send(slots.at[at], slots.at[at], send_sem, recv_sem, *peer).start()

    def ring_sum(slots, recv_sem):
        bytes_of(slots.at[pl.ds(0, SIDE - 1)], recv_sem).wait_recv()
        return (slots[0] + slots[1]) + (slots[2] + slots[3])

    x_peers = [(me, xs[k]) for k in (2, 1, 3)]
    y_peers = [((ys[k] + z) * 2 + core, samp) for k in range(1, SIDE)]
    z_peers = [((y * SIDE + zs[k]) * 2 + core, samp) for k in range(1, SIDE)]

    total = products(0, None)
    tr_core_copy.wait_recv()
    ring_start(tr_own[...] + tr_core[...], tr_x, samp, tr_send.at[1], tr_recv.at[1], x_peers)
    for group in range(1, len(GROUPS)):
        total = products(group, total)

    vp[samp] = total.astype(BF16)
    for peer in x_peers:
        send(vp.at[samp], vp.at[samp], vp_send, vp_recv, *peer).start()
    ring_start(ring_sum(tr_x, tr_recv.at[1]), tr_y, y, tr_send.at[2], tr_recv.at[2], y_peers)
    ring_start(ring_sum(tr_y, tr_recv.at[2]), tr_z, z, tr_send.at[3], tr_recv.at[3], z_peers)
    bytes_of(vp.at[pl.ds(0, XS - 1)], vp_recv).wait_recv()
    grad = vp[0].astype(F32)
    for source in range(1, XS):
        grad = grad + vp[source].astype(F32)
    grad = grad * norm
    score = jnp.sqrt(jnp.sum(grad * grad, axis=0, keepdims=True))
    score = jnp.where(active > 0.0, F32(0.0), score)
    best = score[:, :128]
    for at in range(128, width, 128):
        best = jnp.maximum(best, score[:, at : at + 128])
    tops[2 * HERE + core] = best
    top_own = tops.at[2 * HERE + core]
    for which in range(2):
        for i in range(HERE):
            across(top_own, tops, top_send, top_recv, i, which).start()
    across(top_own, tops, top_send, top_recv, HERE, other).start()
    gv_ref[...] = grad
    score_ref[...] = score
    gt_ref[...] = ring_sum(tr_z, tr_recv.at[3])

    bytes_of(pred_in.at[pl.ds(0, 2 * HERE + 1)], pred_send).wait_send()
    bytes_of(w_in.at[pl.ds(0, 2 * HERE + 1)], w_send).wait_send()
    tr_core_copy.wait_send()
    for k, slots in ((1, tr_x), (2, tr_y), (3, tr_z)):
        bytes_of(slots.at[pl.ds(0, SIDE - 1)], tr_send.at[k]).wait_send()
    bytes_of(vp.at[pl.ds(0, XS - 1)], vp_send).wait_send()
    bytes_of(tops.at[pl.ds(0, 2 * HERE + 1)], top_send).wait_send()
    bytes_of(tops.at[pl.ds(0, 2 * HERE + 1)], top_recv).wait_recv()
    top_ref[...] = jnp.broadcast_to(
        jnp.max(jnp.max(tops[...], axis=0), axis=1, keepdims=True), top_ref.shape
    )


def keep(*refs):
    *refs, sems = refs
    half = len(refs) // 2
    copies = [
        pltpu.make_async_copy(source, target, sems.at[k])
        for k, (source, target) in enumerate(zip(refs[:half], refs[half:]))
    ]
    for copy in copies:
        copy.start()
    for copy in copies:
        copy.wait()


def per_device(genotypes, labels, act_coef, act_index, act_count, loadings, intercept):
    sample_rows, width = genotypes.shape
    rows, traits = labels.shape
    rank = loadings.shape[0]
    slots = act_index.shape[0]
    norm = 1.0 / math.sqrt(sample_rows * lax.axis_size("samp"))
    dma = pltpu.SemaphoreType.DMA
    anywhere = pl.BlockSpec(memory_space=pl.ANY)
    vmem = pl.BlockSpec(memory_space=pltpu.VMEM)
    blocks = (2 * CHIPS, rank, rows)
    trait = (rank, traits)
    in_hbm = functools.partial(pltpu.with_memory_space_constraint, memory_space=pltpu.HBM)
    results = pl.pallas_call(
        functools.partial(kernel, norm),
        out_shape=(
            jax.ShapeDtypeStruct((rank, width), F32),
            jax.ShapeDtypeStruct(trait, F32),
            jax.ShapeDtypeStruct((1, width), F32),
            jax.ShapeDtypeStruct((1, 128), F32),
        ),
        in_specs=[
            *(anywhere,) * 4,
            pl.BlockSpec(memory_space=pltpu.SMEM),
            *(anywhere,) * 2,
        ],
        out_specs=(vmem,) * 4,
        scratch_shapes=[
            pltpu.VMEM((CHIPS, 2 * rows, width), BF16),
            pltpu.VMEM((rows, traits), jnp.int32),
            pltpu.VMEM((rank, slots), BF16),
            pltpu.VMEM((1, slots), jnp.int32),
            pltpu.VMEM(trait, F32),
            pltpu.VMEM((1, traits), F32),
            pltpu.VMEM(blocks, BF16),
            pltpu.VMEM(blocks, BF16),
            pltpu.VMEM(blocks, BF16),
            pltpu.VMEM((XS, rank, width), BF16),
            pltpu.VMEM((2 * CHIPS, 1, 128), F32),
            pltpu.VMEM(trait, F32),
            pltpu.VMEM(trait, F32),
            pltpu.VMEM((XS, *trait), F32),
            pltpu.VMEM((SIDE, *trait), F32),
            pltpu.VMEM((SIDE, *trait), F32),
            dma((len(BATCHES),)),
            dma((5,)),
            dma,
            dma,
            dma,
            dma((len(GROUPS),)),
            dma,
            dma,
            dma,
            dma,
            dma((4,)),
            dma((4,)),
        ],
        compiler_params=pltpu.CompilerParams(
            collective_id=0, has_side_effects=True, vmem_limit_bytes=48 * 1024 * 1024
        ),
    )(
        in_hbm(genotypes),
        in_hbm(labels),
        in_hbm(act_coef),
        in_hbm(act_index.reshape(1, slots)),
        act_count,
        in_hbm(loadings),
        in_hbm(intercept.reshape(1, traits)),
    )
    grad_var, grad_trait, score, top = pl.pallas_call(
        keep,
        out_shape=tuple(jax.ShapeDtypeStruct(x.shape, x.dtype) for x in results),
        in_specs=[anywhere] * len(results),
        out_specs=(anywhere,) * len(results),
        scratch_shapes=[dma((len(results),))],
        compiler_params=pltpu.CompilerParams(vmem_limit_bytes=4 * 1024 * 1024),
    )(*results)
    return grad_var, grad_trait, score.reshape(width), top[0, :1]


def solution(mesh):
    placed = (
        P("samp", "var"),
        P(("samp", "var"), None),
        P(None, "var"),
        P("var"),
        P("var"),
        P(),
        P(),
    )
    return jax.shard_map(
        per_device,
        mesh=mesh,
        in_specs=placed,
        out_specs=(P(None, "var"), P(), P("var"), P()),
        check_vma=False,
    )
```
